32 devices in a mesh: gx: 4 (over z), gy: 8 (over y, x, core).
Axes of the slice: x: 2, y: 2, z: 4, core: 2. Of those that a mesh axis runs over, the one named last changes fastest.
Arguments:
- coordinates: float32 [3, 65536], P(None, ('gx', 'gy')), may hold values from 0 to 1
- rhs: float32 [16, 65536], P(None, ('gx', 'gy')), may hold values from -70 to 70
- leaf_order: int32 [32, 2048], P(('gx', 'gy')), may hold values from 0 to 2047, each once within a row
- leaf_sizes: int32 [32], P(('gx', 'gy')), may hold values from 1 to 2048, 49152 in all
- inverse_scales: float32 [3], replicated, may hold values from 12 to 30
- noise_var: float32 [1], replicated, may hold values from 0.3 to 1
- u_factors: float32 [5, 64, 65536], P(None, None, ('gx', 'gy')), may hold values from -0.375 to 0.375
- v_factors: float32 [5, 64, 65536], P(None, None, ('gx', 'gy')), may hold values from -1 to 1
Outputs:
- solution: float32 [16, 65536], P(None, ('gx', 'gy'))
The draws below stay inside these ranges and needn't reach their ends.
Inputs may be any that keep to these rules, and one draw needn't show every extreme that they name: `leaf_sizes`: each leaf's live points stand first in leaf order.
All inputs are finite; a program needn't handle non-finite values. No bound on the sum of `leaf_sizes` on one device may be relied on, other than what follows from the above.
Results may differ from the reference program's by a relative error of at most 0.0001.
Values sent between devices are 32-bit elements; how exact they have to be, the bound alone decides.
A program may use at most 128 MiB of HBM per device.

```python
import math
import jax
import jax.numpy as jnp
import numpy as np
from jax import lax

LEAF = 2048
RANK = 64
VECTORS = 16
ITERS = 3
LEVELS = 5
LEAVES = 32
POINTS = 65536


def draw_v_factors(key, part):
    key_values = jax.random.fold_in(key, 11)
    level_ids = jnp.arange(LEVELS, dtype=jnp.float32)
    level_scale = 1.0 / jnp.sqrt(LEAF * 2.0 ** level_ids)
    values = jnp.clip(jax.random.normal(key_values, (LEVELS, RANK, POINTS), jnp.float32), -5.0, 5.0)
    return values * level_scale[:, None, None]


def draw_rhs(key, part):
    key_main = jax.random.fold_in(key, 21)
    key_column = jax.random.fold_in(key, 22)
    key_row = jax.random.fold_in(key, 23)
    position = jnp.arange(POINTS, dtype=jnp.float32) / POINTS
    column_scale = jnp.exp(jax.random.uniform(key_column, (1, POINTS), jnp.float32, 0.0, math.log(2.5)))
    row_scale = jnp.exp(jax.random.uniform(key_row, (VECTORS, 1), jnp.float32, math.log(1.0 / 3.0), math.log(10.0 / 3.0)))
    base = jnp.clip(jax.random.normal(key_main, (VECTORS, POINTS), jnp.float32), -4.0, 4.0)
    base = base * 0.5 * jnp.exp(math.log(3.0) * position)[None, :]
    return base * column_scale * row_scale


def levels(rng, shape, shards, low, high):
    def one(dim, parts):
        draws = jax.random.uniform(jax.random.fold_in(jax.random.fold_in(rng, 6), dim), (parts,), jnp.float32, low / len(shards), high / len(shards))
        return jnp.repeat(jnp.exp(draws), shape[dim] // parts).reshape((-1,) + (1,) * (len(shape) - dim - 1))

    gain = one(*shards[0])
    for cut in shards[1:]:
        gain = gain * one(*cut)
    return gain


def profile(amount, total, bound, slope):
    weights = [(1 << 20) // math.isqrt(rank ** slope) + 1 for rank in range(2, amount + 1)]
    rest, counts = total - bound - (amount - 1), [1] * (amount - 1)
    while rest > 0:
        movable = [i for i in range(amount - 1) if counts[i] < bound]
        whole, left = sum([weights[i] for i in movable]), rest
        for i in movable:
            addition = min(bound - counts[i], max(1, left * weights[i] // whole), rest)
            counts[i] = counts[i] + addition
            rest = rest - addition
    return np.array([bound] + counts)


def ragged_sizes(stream_key, amount, total, reach, skew):
    if amount == 2:
        one = jax.random.randint(stream_key, (), max(1, total - reach), min(reach, total - 1) + 1)
        return jnp.stack([one, total - one])
    sizes = jnp.asarray(profile(amount, total, reach, skew), jnp.int32)
    couples = (amount - 1) // 2
    donor, taker = sizes[1:1 + 2 * couples:2], sizes[2:2 + 2 * couples:2]
    room = jnp.minimum(donor - 1, reach - taker)
    shifted = jax.random.randint(jax.random.fold_in(stream_key, 1), (couples,), 0, 1 << 20) % (room + 1)
    sizes = sizes.at[1:1 + 2 * couples:2].set(donor - shifted).at[2:2 + 2 * couples:2].set(taker + shifted)
    return sizes[jax.random.permutation(jax.random.fold_in(stream_key, 2), amount)]


def scatter_about(rng, extent, width, bound, cuts=(), kind=jnp.bfloat16):
    values = jax.random.normal(rng, extent, jnp.float32) * width
    if len(cuts) > 0:
        values = levels(rng, extent, cuts, -0.22, 0.18) * values
    return jnp.clip(values, min=-bound, max=bound).astype(kind)


def setup_inputs(seed: int = 0) -> dict:
    splits = jax.random.split(jax.random.key(seed), 9)
    return {
        "coordinates": jnp.clip(1.0 * jax.random.uniform(splits[0], (3, POINTS), jnp.float32) ** levels(splits[0], (3, POINTS), ((1, 32),), -0.2, 0.2), 0.0, 1.0),
        "rhs": draw_rhs(jax.random.fold_in(splits[8], 71), 0),
        "leaf_order": jax.vmap(lambda own: jax.random.permutation(own, LEAF))(jax.random.split(splits[2], LEAVES)).reshape((LEAVES, LEAF)).astype(jnp.int32),
        "leaf_sizes": ragged_sizes(splits[3], LEAVES, LEAVES * LEAF * 3 // 4, LEAF, 1).astype(jnp.int32),
        "inverse_scales": jnp.clip(jnp.exp(jax.random.uniform(splits[4], (3,), jnp.float32, math.log(12.0), math.log(30.0))), 12.0, 30.0),
        "noise_var": jnp.clip(jnp.exp(jax.random.uniform(splits[5], (1,), jnp.float32, math.log(0.3), math.log(1.0))), 0.3, 1.0),
        "u_factors": scatter_about(splits[6], (LEVELS, RANK, POINTS), (4 * RANK) ** -0.5, 0.375, ((2, 32),), jnp.float32),
        "v_factors": draw_v_factors(jax.random.fold_in(splits[8], 71), 0),
    }


epsilon = 1e-06
sqrt_three = math.sqrt(3.0)
highest = lax.Precision.HIGHEST

def build_kernel(scaled):
    width_all = scaled.shape[1]
    block_rows = min(512, width_all)
    pieces = []
    for start_row in range(0, width_all, block_rows):
        row_points = scaled[:, start_row:start_row + block_rows]
        differ = row_points[:, :, None] - scaled[:, None, :]
        distance = jnp.sqrt(lax.optimization_barrier(jnp.sum(differ * differ, axis=0)))
        pieces.append((1.0 + sqrt_three * distance) * jnp.exp(-sqrt_three * distance))
    return jnp.concatenate(pieces, axis=0)

def least_squares(columns, beta):
    count_cols = len(columns)
    cosines = []
    sines = []
    target = [beta] + [jnp.zeros_like(beta)] * count_cols
    upper = []
    for column_idx in range(count_cols):
        entries = list(columns[column_idx])
        for row_idx in range(column_idx):
            first_val = entries[row_idx]
            second_val = entries[row_idx + 1]
            entries[row_idx] = cosines[row_idx] * first_val + sines[row_idx] * second_val
            entries[row_idx + 1] = -sines[row_idx] * first_val + cosines[row_idx] * second_val
        first_val = entries[column_idx]
        second_val = entries[column_idx + 1]
        radius = jnp.sqrt(first_val * first_val + second_val * second_val)
        cosines.append(first_val / radius)
        sines.append(second_val / radius)
        entries[column_idx] = radius
        carried = target[column_idx]
        target[column_idx] = cosines[column_idx] * carried
        target[column_idx + 1] = -sines[column_idx] * carried
        upper.append(entries[:column_idx + 1])
    weights = [None] * count_cols
    for column_idx in reversed(range(count_cols)):
        accum = target[column_idx]
        for later_idx in range(column_idx + 1, count_cols):
            accum = accum - upper[later_idx][column_idx] * weights[later_idx]
        weights[column_idx] = accum / upper[column_idx][column_idx]
    return weights

def reference(coordinates, rhs, leaf_order, leaf_sizes, inverse_scales, noise_var, u_factors, v_factors):
    num_leaves = leaf_order.shape[0]
    leaf_len = leaf_order.shape[1]
    num_vectors = rhs.shape[0]
    num_levels = u_factors.shape[0]
    num_rank = u_factors.shape[1]
    num_points = num_leaves * leaf_len
    points = jnp.take_along_axis(coordinates.reshape(3, num_leaves, leaf_len), leaf_order[None], axis=2)
    scaled = points * inverse_scales[:, None, None]
    ordered = jnp.take_along_axis(rhs.reshape(num_vectors, num_leaves, leaf_len), leaf_order[None], axis=2)
    live_mask = (jnp.arange(leaf_len, dtype=jnp.int32)[None, :] < leaf_sizes[:, None]).astype(jnp.float32)
    scaled_leaves = jnp.moveaxis(scaled, 1, 0)

    def dense_part(vector):

        def one_leaf(pair):
            leaf_scaled, leaf_vector = pair
            kernel = build_kernel(leaf_scaled)
            return jnp.dot(leaf_vector, kernel, precision=highest)
        result = lax.map(one_leaf, (scaled_leaves, jnp.moveaxis(vector, 1, 0)))
        return jnp.moveaxis(result, 0, 1)

    def low_part(vector):
        flat = vector.reshape(num_vectors, num_points)
        total = jnp.zeros((num_vectors, num_leaves, leaf_len), jnp.float32)
        for level in range(num_levels):
            nodes = num_leaves >> level
            node_len = leaf_len << level
            right_fac = v_factors[level].reshape(num_rank, nodes, node_len)
            coef = jnp.einsum('rnp,knp->nrk', right_fac, flat.reshape(num_vectors, nodes, node_len), precision=highest)
            sibling = coef.reshape(nodes // 2, 2, num_rank, num_vectors)[:, ::-1].reshape(nodes, num_rank, num_vectors)
            left_fac = u_factors[level].reshape(num_rank, nodes, node_len)
            total = total + jnp.einsum('rnp,nrk->knp', left_fac, sibling, precision=highest).reshape(num_vectors, num_leaves, leaf_len)
        return total

    def operate(vector):
        return live_mask[None] * (dense_part(vector) + noise_var[0] * vector + low_part(vector))
    start = live_mask[None] * ordered
    beta = jnp.sqrt(lax.optimization_barrier(jnp.sum(start * start, axis=(1, 2))) + epsilon)
    basis = [start / beta[:, None, None]]
    columns = []
    for step_idx in range(ITERS):
        image = operate(basis[step_idx])
        column = [lax.optimization_barrier(jnp.sum(basis[row_idx] * image, axis=(1, 2))) for row_idx in range(step_idx + 1)]
        for row_idx in range(step_idx + 1):
            image = image - column[row_idx][:, None, None] * basis[row_idx]
        length = jnp.sqrt(lax.optimization_barrier(jnp.sum(image * image, axis=(1, 2))) + epsilon)
        column.append(length)
        columns.append(column)
        if step_idx + 1 < ITERS:
            basis.append(image / length[:, None, None])
    weights = least_squares(columns, beta)
    solved = weights[0][:, None, None] * basis[0]
    for step_idx in range(1, ITERS):
        solved = solved + weights[step_idx][:, None, None] * basis[step_idx]
    leaf_rows = jnp.arange(num_leaves, dtype=jnp.int32)[:, None]
    placed = jnp.zeros((num_vectors, num_leaves, leaf_len), jnp.float32).at[:, leaf_rows, leaf_order].set(solved)
    return placed.reshape(num_vectors, num_points)
```

```python
import functools
import math

import jax
import jax.numpy as jnp
from jax import lax
from jax.experimental import pallas as pl
from jax.experimental.pallas import tpu as pltpu
from jax.sharding import PartitionSpec as P

ITERS = 3

epsilon = 1e-06
sqrt_three = math.sqrt(3.0)
log2_e = math.log2(math.e)
MESH = pl.DeviceIdType.MESH
f32 = jnp.float32
bf16 = jnp.bfloat16
NN = (((1,), (0,)), ((), ()))
NT = (((1,), (1,)), ((), ()))


def least_squares(columns, beta):
    count_cols = len(columns)
    cosines = []
    sines = []
    target = [beta] + [jnp.zeros_like(beta)] * count_cols
    upper = []
    for column_idx in range(count_cols):
        entries = list(columns[column_idx])
        for row_idx in range(column_idx):
            first_val = entries[row_idx]
            second_val = entries[row_idx + 1]
            entries[row_idx] = cosines[row_idx] * first_val + sines[row_idx] * second_val
            entries[row_idx + 1] = -sines[row_idx] * first_val + cosines[row_idx] * second_val
        first_val = entries[column_idx]
        second_val = entries[column_idx + 1]
        radius = jnp.sqrt(first_val * first_val + second_val * second_val)
        cosines.append(first_val / radius)
        sines.append(second_val / radius)
        entries[column_idx] = radius
        carried = target[column_idx]
        target[column_idx] = cosines[column_idx] * carried
        target[column_idx + 1] = -sines[column_idx] * carried
        upper.append(entries[: column_idx + 1])
    weights = [None] * count_cols
    for column_idx in reversed(range(count_cols)):
        accum = target[column_idx]
        for later_idx in range(column_idx + 1, count_cols):
            accum = accum - upper[later_idx][column_idx] * weights[later_idx]
        weights[column_idx] = accum / upper[column_idx][column_idx]
    return weights


def flipped(index, bits):
    result = index
    place = 1
    while place <= bits:
        if bits & place:
            result = result + place * (1 - 2 * lax.rem(lax.div(index, place), 2))
        place *= 2
    return result


def split2(value):
    high = value.astype(bf16)
    low = (value - high.astype(f32)).astype(bf16)
    return high, low


def split3(value):
    high = value.astype(bf16)
    rest = value - high.astype(f32)
    mid = rest.astype(bf16)
    low = (rest - mid.astype(f32)).astype(bf16)
    return high, mid, low


def dot(left, right, dims=NN):
    return lax.dot_general(left, right, dims, preferred_element_type=f32)


def fused(
    size_gx, size_gy,
    coords_ref, rhs_ref, order_ref, sizes_ref, inv_ref, noise_ref, u_hbm, v_hbm,
    out_ref,
    near_hi, near_lo, columns_pos, rows_pos, u_raw, v_raw, u_hi, u_lo, v_hi, v_lo,
    basis_ref, image_ref,
    send_part, recv_low, recv_high, send_node, recv_node,
    send_dots, recv_dots,
    load_sem,
    part_s, part_r, node_s, node_r, dots_s, dots_r,
):
    me_x = lax.axis_index("gx")
    me_y = lax.axis_index("gy")
    levels_low = size_gy.bit_length() - 1
    levels_high = size_gx.bit_length() - 1
    nv, leaf_len = rhs_ref.shape
    num_dims = coords_ref.shape[0]
    num_levels, num_rank = u_raw.shape[0], u_raw.shape[1]
    half = nv // 2
    lanes = 2 * num_rank
    size_all = size_gx * size_gy

    u_load = pltpu.make_async_copy(u_hbm, u_raw, load_sem.at[0])
    v_load = pltpu.make_async_copy(v_hbm, v_raw, load_sem.at[1])
    v_load.start()
    u_load.start()

    peers = [
        (flipped(me_x, apart // size_gy), flipped(me_y, apart % size_gy)) for apart in range(size_all)
    ]
    barrier = pltpu.get_barrier_semaphore()
    for apart in range(1, size_all):
        pl.semaphore_signal(barrier, inc=1, device_id=peers[apart], device_id_type=MESH)

    def send(src, dst, sems, semr, device):
        copy = pltpu.make_async_remote_copy(
            src_ref=src, dst_ref=dst, send_sem=sems, recv_sem=semr,
            device_id=device, device_id_type=MESH,
        )
        copy.start()
        return copy

    live = jnp.where(
        lax.broadcasted_iota(jnp.int32, (1, leaf_len), 1) < sizes_ref[0], 1.0, 0.0
    ).astype(f32)

    width = 128
    groups = leaf_len // width
    order = order_ref[...]
    outer = lax.div(order, width)
    inner = order - outer * width
    pick = jnp.where(
        lax.broadcasted_iota(jnp.int32, (width, leaf_len), 0) == inner, 1.0, 0.0
    ).astype(bf16)

    def gather(value):
        rows = value.shape[0]
        parts = []
        for part in split3(value):
            parts += [part[:, g * width : (g + 1) * width] for g in range(groups)]
        stacked = jnp.concatenate(parts, axis=0)
        pieces = []
        for start_col in range(0, leaf_len, 512):
            cols = slice(start_col, start_col + 512)
            got = dot(stacked, pick[:, cols])
            total = jnp.zeros((rows, 512), f32)
            for g in range(groups):
                terms = [
                    got[(part * groups + g) * rows : (part * groups + g + 1) * rows] for part in range(3)
                ]
                total = jnp.where(outer[:, cols] == g, terms[0] + terms[1] + terms[2], total)
            pieces.append(total)
        return jnp.concatenate(pieces, axis=1)

    pad = jnp.zeros((16 - num_dims, leaf_len), f32)
    row_sel = lax.broadcasted_iota(jnp.int32, (16, 1), 0)
    scale = jnp.zeros((16, 1), f32)
    for dim in range(num_dims):
        scale = jnp.where(row_sel == dim, inv_ref[dim], scale)
    gathered = gather(jnp.concatenate([coords_ref[...], pad], axis=0))
    rows_pos[0:16, :] = gathered * scale * sqrt_three
    rows_pos[16:, :] = jnp.zeros((rows_pos.shape[0] - 16, leaf_len), f32)
    columns_pos[...] = rows_pos[...].T
    basis_ref[0] = live * gather(rhs_ref[...])

    padded = v_hi.shape[0]
    used = num_levels * num_rank

    def prepare(raw, hi, lo):
        for level in range(num_levels):
            first, second = split2(raw[level])
            hi[level * num_rank : (level + 1) * num_rank, :] = first
            lo[level * num_rank : (level + 1) * num_rank, :] = second
        if padded > used:
            hi[used:, :] = jnp.zeros((padded - used, leaf_len), bf16)
            lo[used:, :] = jnp.zeros((padded - used, leaf_len), bf16)

    lane = lax.broadcasted_iota(jnp.int32, (half, lanes), 1)
    left_side = lane < num_rank

    def swap(value):
        return pltpu.roll(value, num_rank, 1)

    def send_partials(it, coef):
        for level in range(num_levels):
            block = coef[:, (level // 2) * lanes : (level // 2 + 1) * lanes]
            top, bottom = block[:half], block[half:]
            if level % 2 == 0:
                tile = jnp.where(left_side, top, swap(bottom))
            else:
                tile = jnp.where(left_side, swap(top), bottom)
            send_part[it, level] = tile
        copies = []
        for apart in range(1, size_gy):
            copies.append(send(
                send_part.at[it, pl.ds(levels_low, levels_high)], recv_high.at[it, apart],
                part_s.at[it, apart, 1], part_r.at[it, apart, 1], peers[apart],
            ))
        late = []
        for apart in range(1, size_gy):
            late.append(send(
                send_part.at[it, apart.bit_length() - 1], recv_low.at[it, apart],
                part_s.at[it, apart, 0], part_r.at[it, apart, 0], peers[apart],
            ))
        return copies, late

    def send_nodes(it, part_copies):
        for copy in part_copies:
            copy.wait_recv()
        total = send_part[it, levels_low:num_levels]
        for apart in range(1, size_gy):
            total = total + recv_high[it, apart]
        send_node[it] = total
        return [
            send(
                send_node.at[it, apart.bit_length() - 1], recv_node.at[it, apart],
                node_s.at[it, apart], node_r.at[it, apart], peers[apart * size_gy],
            )
            for apart in range(1, size_gx)
        ]

    def siblings(it, copies):
        for copy in copies:
            copy.wait_recv()
        tiles = []
        for count, source in ((levels_low, recv_low), (levels_high, recv_node)):
            for level in range(count):
                total = source[it, 2**level]
                for apart in range(2**level + 1, 2 ** (level + 1)):
                    total = total + source[it, apart]
                tiles.append(total)
        if len(tiles) % 2:
            tiles.append(jnp.zeros_like(tiles[0]))
        blocks = []
        for pair in range(len(tiles) // 2):
            even, odd = tiles[2 * pair], tiles[2 * pair + 1]
            top = jnp.where(left_side, even, swap(odd))
            bottom = jnp.where(left_side, swap(even), odd)
            blocks.append(jnp.concatenate([top, bottom], axis=0))
        return jnp.concatenate(blocks, axis=1)

    slots = lanes // nv
    row16 = lax.broadcasted_iota(jnp.int32, (nv, lanes), 0)
    slot16 = lax.broadcasted_iota(jnp.int32, (nv, lanes), 1) - row16 * slots

    def send_sums(it, values):
        block = jnp.zeros((nv, lanes), f32)
        for idx, value in enumerate(values):
            block = jnp.where(slot16 == idx, value, block)
        send_dots[it] = jnp.sum(block, axis=0, keepdims=True)
        return [
            send(
                send_dots.at[it], recv_dots.at[it, apart],
                dots_s.at[it, apart], dots_r.at[it, apart], peers[apart],
            )
            for apart in range(1, size_all)
        ]

    def read_sums(it, copies, count):
        for copy in copies:
            copy.wait_recv()
        terms = [send_dots[it]] + [recv_dots[it, apart] for apart in range(1, size_all)]
        while len(terms) > 1:
            terms = [terms[i] + terms[i + 1] for i in range(0, len(terms), 2)]
        return [
            jnp.sum(jnp.where(slot16 == idx, terms[0], 0.0), axis=1, keepdims=True)
            for idx in range(count)
        ]

    chunk = min(512, leaf_len)

    def near_columns(both, first, begin, end):
        for low in range(begin, end, chunk):
            high = low + chunk
            cols = slice(low, high)
            wide = dot(both[:, :high], near_hi[:high, cols])
            rest = dot(first[:, :high], near_lo[:high, cols])
            if high < leaf_len:
                wide = wide + dot(both[:, high:], near_hi[cols, high:], NT)
                rest = rest + dot(first[:, high:], near_lo[cols, high:], NT)
            image_ref[:, cols] = wide[:nv] + wide[nv:] + rest

    rows = 16

    def fill_near():
        for low in range(0, leaf_len, chunk):
            cols = slice(low, low + chunk)

            def fill(block, carry, cols=cols):
                base = pl.multiple_of(block * rows, rows)
                square = None
                for dim in range(num_dims):
                    differ = columns_pos[pl.ds(base, rows), dim : dim + 1] - rows_pos[dim : dim + 1, cols]
                    square = differ * differ if square is None else square + differ * differ
                distance = square * lax.rsqrt(jnp.maximum(square, 1e-30))
                value = (1.0 + distance) * jnp.exp2(distance * (-log2_e))
                hi, lo = split2(value)
                near_hi[pl.ds(base, rows), cols] = hi
                near_lo[pl.ds(base, rows), cols] = lo
                return carry

            lax.fori_loop(0, (low + chunk) // rows, fill, 0, unroll=4)

    pending = []

    def operate(it, vector):
        first, second = split2(vector)
        both = jnp.concatenate([first, second], axis=0)
        if it == 0:
            v_load.wait()
            prepare(v_raw, v_hi, v_lo)
        wide = dot(both, v_hi[...], NT)
        coef = wide[:nv] + wide[nv:] + dot(first, v_lo[...], NT)
        if it == 0:
            pl.semaphore_wait(barrier, size_all - 1)
        parts, late = send_partials(it, coef)
        if it == 0:
            fill_near()
            u_load.wait()
            prepare(u_raw, u_hi, u_lo)
            nodes = send_nodes(it, parts)
            near_columns(both, first, 0, leaf_len)
        else:
            near_columns(both, first, 0, leaf_len // 2)
            nodes = send_nodes(it, parts)
            near_columns(both, first, leaf_len // 2, leaf_len)
        coef_hi, coef_lo = split2(siblings(it, late + nodes))
        wide = dot(jnp.concatenate([coef_hi, coef_lo], axis=0), u_hi[...])
        far = wide[:nv] + wide[nv:] + dot(coef_hi, u_lo[...])
        pending.extend(parts + late + nodes)
        return live * (image_ref[...] + far) - vector

    def lane_sum(value):
        return jnp.sum(value, axis=1, keepdims=True)

    shift = 1.0 + noise_ref[0]
    gram = {}
    columns = []
    images = []
    beta = None
    raw = basis_ref[0]
    image = operate(0, raw)
    for it in range(ITERS):
        last = it + 1 == ITERS
        values = [lane_sum(basis_ref[row] * image) for row in range(it)] + [lane_sum(raw * image)]
        values += [lane_sum(basis_ref[row] * raw) for row in range(it)] + [lane_sum(raw * raw)]
        if last:
            values.append(lane_sum(image * image))
        copies = send_sums(it, values)
        pending.extend(copies)
        ahead = None if last else operate(it + 1, image)
        sums = read_sums(it, copies, len(values))
        length = jnp.sqrt(sums[2 * it + 1] + epsilon)
        inverse = 1.0 / length
        if it == 0:
            beta = length
        else:
            columns[-1].append(length)
        products = [value * inverse for value in sums[: it + 1]]
        products[it] = products[it] * inverse
        lengths = [value * inverse for value in sums[it + 1 : 2 * it + 2]]
        lengths[it] = lengths[it] * inverse
        vector = raw * inverse
        basis_ref[it] = vector
        for row in range(it + 1):
            gram[row, it] = gram[it, row] = lengths[row]
        column = [products[row] + shift * lengths[row] for row in range(it + 1)]
        moved = [column[row] - shift if row == it else column[row] for row in range(it + 1)]
        columns.append(list(column))
        if last:
            rest = sums[-1] * inverse * inverse
            for row in range(it + 1):
                inside = -2.0 * products[row]
                for other in range(it + 1):
                    inside = inside + moved[other] * gram[row, other]
                rest = rest + moved[row] * inside
            columns[-1].append(jnp.sqrt(jnp.maximum(rest, 0.0) + epsilon))
        else:
            images.append(image * inverse)
            raw = images[it]
            image = ahead * inverse
            for row in range(it + 1):
                raw = raw - moved[row] * basis_ref[row]
                image = image - moved[row] * images[row]
    weights = least_squares(columns, beta)
    solved = weights[0] * basis_ref[0]
    for it in range(1, ITERS):
        solved = solved + weights[it] * basis_ref[it]
    parts = split3(solved)
    for g in range(groups):
        mask = jnp.where(outer == g, 1.0, 0.0).astype(bf16)
        stacked = jnp.concatenate([part * mask for part in parts], axis=0)
        got = dot(stacked, pick, NT)
        out_ref[:, g * width : (g + 1) * width] = got[:nv] + got[nv : 2 * nv] + got[2 * nv :]
    for copy in pending:
        copy.wait_send()


def per_device(
    size_gx, size_gy,
    coordinates, rhs, leaf_order, leaf_sizes, inverse_scales, noise_var, u_factors, v_factors,
):
    num_vectors, leaf_len = rhs.shape
    num_levels, num_rank = u_factors.shape[0], u_factors.shape[1]
    levels_high = size_gx.bit_length() - 1
    half, lanes = num_vectors // 2, 2 * num_rank
    padded = (num_levels + 1) // 2 * 2 * num_rank
    tile = (half, lanes)
    vmem = pl.BlockSpec(memory_space=pltpu.VMEM)
    smem = pl.BlockSpec(memory_space=pltpu.SMEM)
    any_space = pl.BlockSpec(memory_space=pl.ANY)
    dma = pltpu.SemaphoreType.DMA
    return pl.pallas_call(
        functools.partial(fused, size_gx, size_gy),
        out_shape=jax.ShapeDtypeStruct(rhs.shape, f32),
        in_specs=[vmem, vmem, vmem, smem, smem, smem, any_space, any_space],
        out_specs=vmem,
        scratch_shapes=[
            pltpu.VMEM((leaf_len, leaf_len), bf16),
            pltpu.VMEM((leaf_len, leaf_len), bf16),
            pltpu.VMEM((leaf_len, 128), f32),
            pltpu.VMEM((128, leaf_len), f32),
            pltpu.VMEM(u_factors.shape, f32),
            pltpu.VMEM(v_factors.shape, f32),
            pltpu.VMEM((padded, leaf_len), bf16),
            pltpu.VMEM((padded, leaf_len), bf16),
            pltpu.VMEM((padded, leaf_len), bf16),
            pltpu.VMEM((padded, leaf_len), bf16),
            pltpu.VMEM((ITERS,) + rhs.shape, f32),
            pltpu.VMEM(rhs.shape, f32),
            pltpu.VMEM((ITERS, num_levels) + tile, f32),
            pltpu.VMEM((ITERS, size_gy) + tile, f32),
            pltpu.VMEM((ITERS, size_gy, levels_high) + tile, f32),
            pltpu.VMEM((ITERS, levels_high) + tile, f32),
            pltpu.VMEM((ITERS, size_gx) + tile, f32),
            pltpu.VMEM((ITERS, 1, lanes), f32),
            pltpu.VMEM((ITERS, size_gx * size_gy, 1, lanes), f32),
            dma((2,)),
            dma((ITERS, size_gy, 2)),
            dma((ITERS, size_gy, 2)),
            dma((ITERS, size_gx)),
            dma((ITERS, size_gx)),
            dma((ITERS, size_gx * size_gy)),
            dma((ITERS, size_gx * size_gy)),
        ],
        compiler_params=pltpu.CompilerParams(collective_id=0, has_side_effects=True),
        name="gmres",
    )(coordinates, rhs, leaf_order, leaf_sizes, inverse_scales, noise_var, u_factors, v_factors)


def solution(mesh):
    in_specs = (
        P(None, ("gx", "gy")),
        P(None, ("gx", "gy")),
        P(("gx", "gy"), None),
        P(("gx", "gy")),
        P(),
        P(),
        P(None, None, ("gx", "gy")),
        P(None, None, ("gx", "gy")),
    )
    out_specs = P(None, ("gx", "gy"))
    return jax.shard_map(
        functools.partial(per_device, mesh.shape["gx"], mesh.shape["gy"]),
        mesh=mesh, in_specs=in_specs, out_specs=out_specs, check_vma=False,
    )
```

```python
import functools
import math

import jax
import jax.numpy as jnp
from jax import lax
from jax.experimental import pallas as pl
from jax.experimental.pallas import tpu as pltpu
from jax.sharding import PartitionSpec as P

ITERS = 3

epsilon = 1e-06
sqrt_three = math.sqrt(3.0)
log2_e = math.log2(math.e)
MESH = pl.DeviceIdType.MESH
f32 = jnp.float32
bf16 = jnp.bfloat16
NN = (((1,), (0,)), ((), ()))
NT = (((1,), (1,)), ((), ()))


def least_squares(columns, beta):
    count_cols = len(columns)
    cosines = []
    sines = []
    target = [beta] + [jnp.zeros_like(beta)] * count_cols
    upper = []
    for column_idx in range(count_cols):
        entries = list(columns[column_idx])
        for row_idx in range(column_idx):
            first_val = entries[row_idx]
            second_val = entries[row_idx + 1]
            entries[row_idx] = cosines[row_idx] * first_val + sines[row_idx] * second_val
            entries[row_idx + 1] = -sines[row_idx] * first_val + cosines[row_idx] * second_val
        first_val = entries[column_idx]
        second_val = entries[column_idx + 1]
        radius = jnp.sqrt(first_val * first_val + second_val * second_val)
        cosines.append(first_val / radius)
        sines.append(second_val / radius)
        entries[column_idx] = radius
        carried = target[column_idx]
        target[column_idx] = cosines[column_idx] * carried
        target[column_idx + 1] = -sines[column_idx] * carried
        upper.append(entries[: column_idx + 1])
    weights = [None] * count_cols
    for column_idx in reversed(range(count_cols)):
        accum = target[column_idx]
        for later_idx in range(column_idx + 1, count_cols):
            accum = accum - upper[later_idx][column_idx] * weights[later_idx]
        weights[column_idx] = accum / upper[column_idx][column_idx]
    return weights


def flipped(index, bits):
    result = index
    place = 1
    while place <= bits:
        if bits & place:
            result = result + place * (1 - 2 * lax.rem(lax.div(index, place), 2))
        place *= 2
    return result


def split2(value):
    high = value.astype(bf16)
    low = (value - high.astype(f32)).astype(bf16)
    return high, low


def split3(value):
    high = value.astype(bf16)
    rest = value - high.astype(f32)
    mid = rest.astype(bf16)
    low = (rest - mid.astype(f32)).astype(bf16)
    return high, mid, low


def dot(left, right, dims=NN):
    return lax.dot_general(left, right, dims, preferred_element_type=f32)


def fused(
    size_gx, size_gy,
    coords_ref, rhs_ref, order_ref, sizes_ref, inv_ref, noise_ref, u_hbm, v_hbm,
    out_ref,
    near_hi, near_lo, columns_pos, rows_pos, u_raw, v_raw, u_hi, u_lo, v_hi, v_lo,
    basis_ref, image_ref,
    send_part, recv_low, recv_high, send_node, recv_node,
    send_dots, recv_dots,
    load_sem,
    part_s, part_r, node_s, node_r, dots_s, dots_r,
):
    me_x = lax.axis_index("gx")
    me_y = lax.axis_index("gy")
    levels_low = size_gy.bit_length() - 1
    levels_high = size_gx.bit_length() - 1
    nv, leaf_len = rhs_ref.shape
    num_dims = coords_ref.shape[0]
    num_levels, num_rank = u_raw.shape[0], u_raw.shape[1]
    half = nv // 2
    lanes = 2 * num_rank
    size_all = size_gx * size_gy

    u_load = pltpu.make_async_copy(u_hbm, u_raw, load_sem.at[0])
    v_load = pltpu.make_async_copy(v_hbm, v_raw, load_sem.at[1])
    v_load.start()
    u_load.start()

    peers = [
        (flipped(me_x, apart // size_gy), flipped(me_y, apart % size_gy)) for apart in range(size_all)
    ]
    barrier = pltpu.get_barrier_semaphore()
    for apart in range(1, size_all):
        pl.semaphore_signal(barrier, inc=1, device_id=peers[apart], device_id_type=MESH)

    def send(src, dst, sems, semr, device):
        copy = pltpu.make_async_remote_copy(
            src_ref=src, dst_ref=dst, send_sem=sems, recv_sem=semr,
            device_id=device, device_id_type=MESH,
        )
        copy.start()
        return copy

    live = jnp.where(
        lax.broadcasted_iota(jnp.int32, (1, leaf_len), 1) < sizes_ref[0], 1.0, 0.0
    ).astype(f32)

    width = 128
    groups = leaf_len // width
    order = order_ref[...]
    outer = lax.div(order, width)
    inner = order - outer * width
    pick = jnp.where(
        lax.broadcasted_iota(jnp.int32, (width, leaf_len), 0) == inner, 1.0, 0.0
    ).astype(bf16)

    def gather(value):
        rows = value.shape[0]
        parts = []
        for part in split3(value):
            parts += [part[:, g * width : (g + 1) * width] for g in range(groups)]
        stacked = jnp.concatenate(parts, axis=0)
        pieces = []
        for start_col in range(0, leaf_len, 512):
            cols = slice(start_col, start_col + 512)
            got = dot(stacked, pick[:, cols])
            total = jnp.zeros((rows, 512), f32)
            for g in range(groups):
                terms = [
                    got[(part * groups + g) * rows : (part * groups + g + 1) * rows] for part in range(3)
                ]
                total = jnp.where(outer[:, cols] == g, terms[0] + terms[1] + terms[2], total)
            pieces.append(total)
        return jnp.concatenate(pieces, axis=1)

    pad = jnp.zeros((16 - num_dims, leaf_len), f32)
    row_sel = lax.broadcasted_iota(jnp.int32, (16, 1), 0)
    scale = jnp.zeros((16, 1), f32)
    for dim in range(num_dims):
        scale = jnp.where(row_sel == dim, inv_ref[dim], scale)
    gathered = gather(jnp.concatenate([coords_ref[...], pad], axis=0))
    rows_pos[0:16, :] = gathered * scale * sqrt_three
    rows_pos[16:, :] = jnp.zeros((rows_pos.shape[0] - 16, leaf_len), f32)
    columns_pos[...] = rows_pos[...].T
    basis_ref[0] = live * gather(rhs_ref[...])

    padded = v_hi.shape[0]
    used = num_levels * num_rank

    def prepare(raw, hi, lo):
        for level in range(num_levels):
            first, second = split2(raw[level])
            hi[level * num_rank : (level + 1) * num_rank, :] = first
            lo[level * num_rank : (level + 1) * num_rank, :] = second
        if padded > used:
            hi[used:, :] = jnp.zeros((padded - used, leaf_len), bf16)
            lo[used:, :] = jnp.zeros((padded - used, leaf_len), bf16)

    lane = lax.broadcasted_iota(jnp.int32, (half, lanes), 1)
    left_side = lane < num_rank

    def swap(value):
        return pltpu.roll(value, num_rank, 1)

    def send_partials(it, coef):
        for level in range(num_levels):
            block = coef[:, (level // 2) * lanes : (level // 2 + 1) * lanes]
            top, bottom = block[:half], block[half:]
            if level % 2 == 0:
                tile = jnp.where(left_side, top, swap(bottom))
            else:
                tile = jnp.where(left_side, swap(top), bottom)
            send_part[it, level] = tile
        copies = []
        for apart in range(1, size_gy):
            copies.append(send(
                send_part.at[it, pl.ds(levels_low, levels_high)], recv_high.at[it, apart],
                part_s.at[it, apart, 1], part_r.at[it, apart, 1], peers[apart],
            ))
        late = []
        for apart in range(1, size_gy):
            late.append(send(
                send_part.at[it, apart.bit_length() - 1], recv_low.at[it, apart],
                part_s.at[it, apart, 0], part_r.at[it, apart, 0], peers[apart],
            ))
        return copies, late

    def send_nodes(it, part_copies):
        for copy in part_copies:
            copy.wait_recv()
        total = send_part[it, levels_low:num_levels]
        for apart in range(1, size_gy):
            total = total + recv_high[it, apart]
        send_node[it] = total
        return [
            send(
                send_node.at[it, apart.bit_length() - 1], recv_node.at[it, apart],
                node_s.at[it, apart], node_r.at[it, apart], peers[apart * size_gy],
            )
            for apart in range(1, size_gx)
        ]

    def siblings(it, copies):
        for copy in copies:
            copy.wait_recv()
        tiles = []
        for count, source in ((levels_low, recv_low), (levels_high, recv_node)):
            for level in range(count):
                total = source[it, 2**level]
                for apart in range(2**level + 1, 2 ** (level + 1)):
                    total = total + source[it, apart]
                tiles.append(total)
        if len(tiles) % 2:
            tiles.append(jnp.zeros_like(tiles[0]))
        blocks = []
        for pair in range(len(tiles) // 2):
            even, odd = tiles[2 * pair], tiles[2 * pair + 1]
            top = jnp.where(left_side, even, swap(odd))
            bottom = jnp.where(left_side, swap(even), odd)
            blocks.append(jnp.concatenate([top, bottom], axis=0))
        return jnp.concatenate(blocks, axis=1)

    slots = lanes // nv
    row16 = lax.broadcasted_iota(jnp.int32, (nv, lanes), 0)
    slot16 = lax.broadcasted_iota(jnp.int32, (nv, lanes), 1) - row16 * slots

    def send_sums(it, values):
        block = jnp.zeros((nv, lanes), f32)
        for idx, value in enumerate(values):
            block = jnp.where(slot16 == idx, value, block)
        send_dots[it] = jnp.sum(block, axis=0, keepdims=True)
        return [
            send(
                send_dots.at[it], recv_dots.at[it, apart],
                dots_s.at[it, apart], dots_r.at[it, apart], peers[apart],
            )
            for apart in range(1, size_all)
        ]

    def read_sums(it, copies, count):
        for copy in copies:
            copy.wait_recv()
        terms = [send_dots[it]] + [recv_dots[it, apart] for apart in range(1, size_all)]
        while len(terms) > 1:
            terms = [terms[i] + terms[i + 1] for i in range(0, len(terms), 2)]
        return [
            jnp.sum(jnp.where(slot16 == idx, terms[0], 0.0), axis=1, keepdims=True)
            for idx in range(count)
        ]

    chunk = min(512, leaf_len)

    def near_columns(both, first, begin, end):
        for low in range(begin, end, chunk):
            high = low + chunk
            cols = slice(low, high)
            wide = dot(both[:, :high], near_hi[:high, cols])
            rest = dot(first[:, :high], near_lo[:high, cols])
            if high < leaf_len:
                wide = wide + dot(both[:, high:], near_hi[cols, high:], NT)
                rest = rest + dot(first[:, high:], near_lo[cols, high:], NT)
            image_ref[:, cols] = wide[:nv] + wide[nv:] + rest

    rows = 16

    def fill_near(begin, end):
        for low in range(begin, end, chunk):
            cols = slice(low, low + chunk)

            def fill(block, carry, cols=cols):
                base = pl.multiple_of(block * rows, rows)
                square = None
                for dim in range(num_dims):
                    differ = columns_pos[pl.ds(base, rows), dim : dim + 1] - rows_pos[dim : dim + 1, cols]
                    square = differ * differ if square is None else square + differ * differ
                distance = square * lax.rsqrt(jnp.maximum(square, 1e-30))
                value = (1.0 + distance) * jnp.exp2(distance * (-log2_e))
                hi, lo = split2(value)
                near_hi[pl.ds(base, rows), cols] = hi
                near_lo[pl.ds(base, rows), cols] = lo
                return carry

            lax.fori_loop(0, (low + chunk) // rows, fill, 0, unroll=16)

    pending = []

    def operate(it, vector):
        first, second = split2(vector)
        both = jnp.concatenate([first, second], axis=0)
        if it == 0:
            v_load.wait()
            prepare(v_raw, v_hi, v_lo)
        wide = dot(both, v_hi[...], NT)
        coef = wide[:nv] + wide[nv:] + dot(first, v_lo[...], NT)
        if it == 0:
            pl.semaphore_wait(barrier, size_all - 1)
        parts, late = send_partials(it, coef)
        if it == 0:
            fill_near(0, leaf_len - chunk)
            nodes = send_nodes(it, parts)
            fill_near(leaf_len - chunk, leaf_len)
            u_load.wait()
            prepare(u_raw, u_hi, u_lo)
            near_columns(both, first, 0, leaf_len)
        else:
            near_columns(both, first, 0, leaf_len // 2)
            nodes = send_nodes(it, parts)
            near_columns(both, first, leaf_len // 2, leaf_len)
        coef_hi, coef_lo = split2(siblings(it, late + nodes))
        wide = dot(jnp.concatenate([coef_hi, coef_lo], axis=0), u_hi[...])
        far = wide[:nv] + wide[nv:] + dot(coef_hi, u_lo[...])
        pending.extend(parts + late + nodes)
        return live * (image_ref[...] + far) - vector

    def lane_sum(value):
        return jnp.sum(value, axis=1, keepdims=True)

    shift = 1.0 + noise_ref[0]
    gram = {}
    columns = []
    images = []
    beta = None
    raw = basis_ref[0]
    image = operate(0, raw)
    for it in range(ITERS):
        last = it + 1 == ITERS
        values = [lane_sum(basis_ref[row] * image) for row in range(it)] + [lane_sum(raw * image)]
        values += [lane_sum(basis_ref[row] * raw) for row in range(it)] + [lane_sum(raw * raw)]
        if last:
            values.append(lane_sum(image * image))
        copies = send_sums(it, values)
        if last:
            for copy in pending:
                copy.wait_send()
            pending = []
            ahead = None
        else:
            ahead = operate(it + 1, image)
        pending.extend(copies)
        sums = read_sums(it, copies, len(values))
        length = jnp.sqrt(sums[2 * it + 1] + epsilon)
        inverse = 1.0 / length
        if it == 0:
            beta = length
        else:
            columns[-1].append(length)
        products = [value * inverse for value in sums[: it + 1]]
        products[it] = products[it] * inverse
        lengths = [value * inverse for value in sums[it + 1 : 2 * it + 2]]
        lengths[it] = lengths[it] * inverse
        vector = raw * inverse
        basis_ref[it] = vector
        for row in range(it + 1):
            gram[row, it] = gram[it, row] = lengths[row]
        column = [products[row] + shift * lengths[row] for row in range(it + 1)]
        moved = [column[row] - shift if row == it else column[row] for row in range(it + 1)]
        columns.append(list(column))
        if last:
            rest = sums[-1] * inverse * inverse
            for row in range(it + 1):
                inside = -2.0 * products[row]
                for other in range(it + 1):
                    inside = inside + moved[other] * gram[row, other]
                rest = rest + moved[row] * inside
            columns[-1].append(jnp.sqrt(jnp.maximum(rest, 0.0) + epsilon))
        else:
            images.append(image * inverse)
            raw = images[it]
            image = ahead * inverse
            for row in range(it + 1):
                raw = raw - moved[row] * basis_ref[row]
                image = image - moved[row] * images[row]
    weights = least_squares(columns, beta)
    solved = weights[0] * basis_ref[0]
    for it in range(1, ITERS):
        solved = solved + weights[it] * basis_ref[it]
    parts = split3(solved)
    for g in range(groups):
        mask = jnp.where(outer == g, 1.0, 0.0).astype(bf16)
        stacked = jnp.concatenate([part * mask for part in parts], axis=0)
        got = dot(stacked, pick, NT)
        out_ref[:, g * width : (g + 1) * width] = got[:nv] + got[nv : 2 * nv] + got[2 * nv :]
    for copy in pending:
        copy.wait_send()


def per_device(
    size_gx, size_gy,
    coordinates, rhs, leaf_order, leaf_sizes, inverse_scales, noise_var, u_factors, v_factors,
):
    num_vectors, leaf_len = rhs.shape
    num_levels, num_rank = u_factors.shape[0], u_factors.shape[1]
    levels_high = size_gx.bit_length() - 1
    half, lanes = num_vectors // 2, 2 * num_rank
    padded = (num_levels + 1) // 2 * 2 * num_rank
    tile = (half, lanes)
    vmem = pl.BlockSpec(memory_space=pltpu.VMEM)
    smem = pl.BlockSpec(memory_space=pltpu.SMEM)
    any_space = pl.BlockSpec(memory_space=pl.ANY)
    dma = pltpu.SemaphoreType.DMA
    return pl.pallas_call(
        functools.partial(fused, size_gx, size_gy),
        out_shape=jax.ShapeDtypeStruct(rhs.shape, f32),
        in_specs=[vmem, vmem, vmem, smem, smem, smem, any_space, any_space],
        out_specs=vmem,
        scratch_shapes=[
            pltpu.VMEM((leaf_len, leaf_len), bf16),
            pltpu.VMEM((leaf_len, leaf_len), bf16),
            pltpu.VMEM((leaf_len, 128), f32),
            pltpu.VMEM((128, leaf_len), f32),
            pltpu.VMEM(u_factors.shape, f32),
            pltpu.VMEM(v_factors.shape, f32),
            pltpu.VMEM((padded, leaf_len), bf16),
            pltpu.VMEM((padded, leaf_len), bf16),
            pltpu.VMEM((padded, leaf_len), bf16),
            pltpu.VMEM((padded, leaf_len), bf16),
            pltpu.VMEM((ITERS,) + rhs.shape, f32),
            pltpu.VMEM(rhs.shape, f32),
            pltpu.VMEM((ITERS, num_levels) + tile, f32),
            pltpu.VMEM((ITERS, size_gy) + tile, f32),
            pltpu.VMEM((ITERS, size_gy, levels_high) + tile, f32),
            pltpu.VMEM((ITERS, levels_high) + tile, f32),
            pltpu.VMEM((ITERS, size_gx) + tile, f32),
            pltpu.VMEM((ITERS, 1, lanes), f32),
            pltpu.VMEM((ITERS, size_gx * size_gy, 1, lanes), f32),
            dma((2,)),
            dma((ITERS, size_gy, 2)),
            dma((ITERS, size_gy, 2)),
            dma((ITERS, size_gx)),
            dma((ITERS, size_gx)),
            dma((ITERS, size_gx * size_gy)),
            dma((ITERS, size_gx * size_gy)),
        ],
        compiler_params=pltpu.CompilerParams(collective_id=0, has_side_effects=True),
        name="gmres",
    )(coordinates, rhs, leaf_order, leaf_sizes, inverse_scales, noise_var, u_factors, v_factors)


def solution(mesh):
    in_specs = (
        P(None, ("gx", "gy")),
        P(None, ("gx", "gy")),
        P(("gx", "gy"), None),
        P(("gx", "gy")),
        P(),
        P(),
        P(None, None, ("gx", "gy")),
        P(None, None, ("gx", "gy")),
    )
    out_specs = P(None, ("gx", "gy"))
    return jax.shard_map(
        functools.partial(per_device, mesh.shape["gx"], mesh.shape["gy"]),
        mesh=mesh, in_specs=in_specs, out_specs=out_specs, check_vma=False,
    )
```
